32 devices in a mesh: blk: 16 (over z, y, core), head: 2 (over x).
Axes of the slice: x: 2, y: 2, z: 4, core: 2. Of those that a mesh axis runs over, the one named last changes fastest.
Arguments:
- tokens: bfloat16 [2048, 3584], P(('blk', 'head')), may hold values from -100 to 100
- norm_gain: float32 [3584], replicated, may hold values from 0.1 to 1.9
- w_query: bfloat16 [3584, 3072], P('blk', 'head'), may hold values from -0.09375 to 0.09375
- w_key: bfloat16 [3584, 512], P('blk'), may hold values from -0.09375 to 0.09375
- w_value: bfloat16 [3584, 512], P('blk'), may hold values from -0.09375 to 0.09375
- q_bias: float32 [3072], P('head'), may hold values from -200 to 200
- k_bias: float32 [512], replicated, may hold values from -25 to 25
- v_bias: float32 [512], replicated, may hold values from -2.5 to 2.5
- w_out: bfloat16 [3072, 3584], P('head', 'blk'), may hold values from -0.109375 to 0.109375
Outputs:
- attention_out: bfloat16 [2048, 3584], P(('blk', 'head'))
The draws below stay inside these ranges and needn't reach their ends.
All inputs are finite; a program needn't handle non-finite values.
Results may differ from the reference program's by a relative error of at most 0.04.
The reference program's roundings to bfloat16 on the way count: a program that leaves them out, or rounds other values in their place, can miss the bound.
Values may be sent and summed in bfloat16 or wider, within the bound.
A program may use at most 64 MiB of HBM per device.

```python
import jax
import jax.numpy as jnp
from jax import lax

D = 3584
HD = 128
H = 24
G = 6
KVH = 4
SEQ = 2048


def draw_tokens(key, part):
    first, second, third = jax.random.split(jax.random.fold_in(key, 5), 3)
    row_scale = jnp.exp(jax.random.uniform(second, (SEQ, 1), minval=0.0, maxval=jnp.log(10.0)))
    col_scale = jnp.exp(jax.random.uniform(third, (1, D), minval=jnp.log(0.3), maxval=jnp.log(3.0)))
    base = jax.random.normal(first, (SEQ, D))
    return jnp.clip(base * row_scale * col_scale, -100.0, 100.0).astype(jnp.bfloat16)


def draw_q_bias(key, part):
    values = 0.5 * jax.random.normal(jax.random.fold_in(key, 3), (H * HD,))
    return jnp.clip(values, -2.0, 2.0).astype(jnp.float32)


def draw_k_bias(key, part):
    values = 0.5 * jax.random.normal(jax.random.fold_in(key, 4), (KVH * HD,))
    return jnp.clip(values, -2.0, 2.0).astype(jnp.float32)


def shard_levels(key, extent, cuts, least, largest):
    def one(axis_at, shards_of):
        steps = jax.random.uniform(jax.random.fold_in(jax.random.fold_in(key, 6), axis_at), (shards_of,), jnp.float32, least / len(cuts), largest / len(cuts))
        return jnp.repeat(jnp.exp(steps), extent[axis_at] // shards_of).reshape((-1,) + (1,) * (len(extent) - axis_at - 1))

    gain = one(*cuts[0])
    for cut in cuts[1:]:
        gain = gain * one(*cut)
    return gain


def normal_values(key, dims, scale, limit, cuts=(), kind=jnp.bfloat16):
    level = shard_levels(key, dims, cuts, -0.22, 0.18) if cuts else 1.0
    values = jax.random.normal(key, dims, jnp.float32) * scale * level
    return jnp.minimum(jnp.maximum(values, -limit), limit).astype(kind)


def setup_inputs(seed: int = 0) -> dict:
    key_list = jax.random.split(jax.random.key(seed), 10)
    tokens = draw_tokens(jax.random.fold_in(key_list[9], 71), 0)
    norm_gain = jnp.clip(1.0 + 0.18 * jax.random.normal(key_list[1], (D,), jnp.float32), 0.1, 1.9)
    w_query = normal_values(key_list[2], (D, H * HD), D ** -0.5, 0.09375, ((0, 16), (1, 2)))
    w_key = normal_values(key_list[3], (D, KVH * HD), D ** -0.5, 0.09375, ((0, 16),))
    w_value = normal_values(key_list[4], (D, KVH * HD), D ** -0.5, 0.09375, ((0, 16),))
    q_bias = draw_q_bias(jax.random.fold_in(key_list[9], 71), 0)
    k_bias = draw_k_bias(jax.random.fold_in(key_list[9], 71), 0)
    v_bias = normal_values(key_list[7], (KVH * HD,), 0.5, 2.5, (), jnp.float32)
    w_out = normal_values(key_list[8], (H * HD, D), (H * HD) ** -0.5, 0.109375, ((0, 2), (1, 16)))
    return {"tokens": tokens, "norm_gain": norm_gain, "w_query": w_query, "w_key": w_key, "w_value": w_value, "q_bias": q_bias, "k_bias": k_bias, "v_bias": v_bias, "w_out": w_out}


theta_base = 1000000.0
eps_norm = 1e-06
masked_score = -1e+30

def rotary_tables(positions, width):
    half = width // 2
    freq = theta_base ** (-(jnp.arange(half, dtype=jnp.float32) * 2.0 / width))
    angles = positions.astype(jnp.float32)[:, None] * freq[None, :]
    angles = jnp.concatenate([angles, angles], axis=1)
    return (jnp.cos(angles), jnp.sin(angles))

def rotate(values, cosine, sine):
    half = values.shape[-1] // 2
    turned = jnp.concatenate([-values[..., half:], values[..., :half]], axis=-1)
    return values * cosine[:, None, :] + turned * sine[:, None, :]

def reference(tokens, norm_gain, w_query, w_key, w_value, q_bias, k_bias, v_bias, w_out):
    seq_len = tokens.shape[0]
    floats = tokens.astype(jnp.float32)
    normed = (floats * lax.rsqrt(lax.optimization_barrier(jnp.mean(floats * floats, axis=1, keepdims=True)) + eps_norm) * norm_gain).astype(jnp.bfloat16)
    cosine, sine = rotary_tables(jnp.arange(seq_len, dtype=jnp.int32), HD)
    query = jnp.dot(normed, w_query, preferred_element_type=jnp.float32) + q_bias
    query = rotate(query.reshape(seq_len, H, HD), cosine, sine).astype(jnp.bfloat16)
    key = jnp.dot(normed, w_key, preferred_element_type=jnp.float32) + k_bias
    key = rotate(key.reshape(seq_len, KVH, HD), cosine, sine).astype(jnp.bfloat16)
    value = (jnp.dot(normed, w_value, preferred_element_type=jnp.float32) + v_bias).astype(jnp.bfloat16)
    value = value.reshape(seq_len, KVH, HD)
    width = min(512, seq_len)
    block_total = seq_len // width
    scale = 1.0 / HD ** 0.5
    key_positions = jnp.arange(seq_len, dtype=jnp.int32)

    def one_group(group):
        query_group = lax.dynamic_slice_in_dim(query, (group * G).astype(jnp.int32), G, 1)
        key_group = lax.dynamic_index_in_dim(key, group, 1, keepdims=False).astype(jnp.float32)
        value_group = lax.dynamic_index_in_dim(value, group, 1, keepdims=False).astype(jnp.float32)

        def one_block(block):
            start = (block * width).astype(jnp.int32)
            rows_block = lax.dynamic_slice_in_dim(query_group, start, width, 0).astype(jnp.float32)
            scores = jnp.einsum('qhd,kd->hqk', rows_block, key_group) * scale
            query_positions = start + jnp.arange(width, dtype=jnp.int32)
            visible = key_positions[None, :] <= query_positions[:, None]
            scores = jnp.where(visible[None], scores, masked_score)
            top = lax.optimization_barrier(jnp.max(scores, axis=2, keepdims=True))
            weights = jnp.where(visible[None], jnp.exp(scores - top), 0.0)
            total = lax.optimization_barrier(jnp.sum(weights, axis=2))
            rounded = lax.optimization_barrier(weights.astype(jnp.bfloat16))
            mixed = jnp.einsum('hqk,kd->hqd', rounded.astype(jnp.float32), value_group)
            return (mixed / total[..., None]).astype(jnp.bfloat16)
        return lax.map(one_block, jnp.arange(block_total, dtype=jnp.int32))
    outs = lax.map(one_group, jnp.arange(KVH, dtype=jnp.int32))
    attended = outs.transpose(1, 3, 0, 2, 4).reshape(seq_len, H * HD)
    return jnp.dot(attended, w_out, preferred_element_type=jnp.float32).astype(jnp.bfloat16)
```

```python
import functools
import math

import jax
import jax.numpy as jnp
from jax import lax
from jax.experimental import pallas as pl
from jax.experimental.pallas import tpu as pltpu
from jax.sharding import PartitionSpec as P

HD = 128
G = 6
MESH = pl.DeviceIdType.MESH

theta_base = 1000000.0
eps_norm = 1e-06
masked_score = -1e30

WQ, WKV, WO, KV = range(4)
UP, DOWN, ACROSS, CORE = range(4)


def block_width(rows, limit):
    width = min(rows, limit)
    while rows % width:
        width -= 1
    return width


def kernel(
    sizes,
    tokens_ref,
    gain_ref,
    w_query_ref,
    w_key_ref,
    w_value_ref,
    q_bias_ref,
    k_bias_ref,
    v_bias_ref,
    w_out_ref,
    cos_ref,
    sin_ref,
    out_ref,
    wq,
    wkv,
    wo,
    kv,
    normed,
    query,
    attended,
    partial,
    outgoing,
    incoming,
    local_sem,
    send_sem,
    recv_sem,
    norm_send,
    norm_recv,
    sum_send,
    sum_recv,
):
    blocks, heads = sizes
    nz = blocks // 4
    me = lax.axis_index("blk")
    head = lax.axis_index("head")
    z, y, c = me // 4, (me // 2) % 2, me % 2
    local_rows, width = tokens_ref.shape
    group_rows = local_rows * heads
    heads_here = wq.shape[1] // HD
    kv_here = wkv.shape[1] // (2 * HD)
    per_kv = heads_here // kv_here
    kv_cols = kv_here * HD
    kv_start = pl.multiple_of((head * heads_here // G) * HD, HD)
    buffers = {WQ: wq, WKV: wkv, WO: wo, KV: kv}
    scale = 1.0 / math.sqrt(HD)

    def slot_of(zz, yy, cc):
        return (zz * 2 + yy) * 2 + cc

    def rows_of(item, slot):
        each = buffers[item].shape[0] // blocks
        return buffers[item].at[pl.ds(pl.multiple_of(slot * each, each), each)]

    def target(route):
        step = {UP: 4, DOWN: -4, ACROSS: 2 - 4 * y, CORE: 1 - 2 * c}[route]
        return (me + step, head)

    def copy(item, slot, route):
        part = rows_of(item, slot)
        return pltpu.make_async_remote_copy(
            src_ref=part,
            dst_ref=part,
            send_sem=send_sem.at[item, slot, route],
            recv_sem=recv_sem.at[item, slot],
            device_id=target(route),
            device_id_type=MESH,
        )

    def send(item, slot, route):
        if route == UP:
            pl.when(z < nz - 1)(lambda: copy(item, slot, route).start())
        elif route == DOWN:
            pl.when(z > 0)(lambda: copy(item, slot, route).start())
        else:
            copy(item, slot, route).start()

    def sent(item, slot, route):
        if route == UP:
            pl.when(z < nz - 1)(lambda: copy(item, slot, route).wait_send())
        elif route == DOWN:
            pl.when(z > 0)(lambda: copy(item, slot, route).wait_send())
        else:
            copy(item, slot, route).wait_send()

    def arrived(item, slot):
        copy(item, slot, CORE).wait_recv()

    def below(k, act):
        pl.when(z >= k)(lambda: act(z - k))

    def above(k, act):
        pl.when(z + k < nz)(lambda: act(z + k))

    def z_step(item, k, yy, then=()):
        def from_below(zz):
            slot = slot_of(zz, yy, c)
            arrived(item, slot)
            for route in (UP,) + then:
                send(item, slot, route)

        def from_above(zz):
            slot = slot_of(zz, yy, c)
            arrived(item, slot)
            for route in (DOWN,) + then:
                send(item, slot, route)

        below(k, from_below)
        above(k, from_above)

    def at_distance(k, act):
        if k == 0:
            act(z)
        else:
            below(k, act)
            above(k, act)

    def across(item, k):
        def act(zz):
            slot = slot_of(zz, 1 - y, c)
            arrived(item, slot)
            send(item, slot, CORE)

        at_distance(k, act)

    def finish(item):
        for zz in range(nz):
            for yy in range(2):
                arrived(item, slot_of(zz, yy, 1 - c))

    def drain(item, both):
        for yy in (y, 1 - y) if both else (y,):
            for route in (UP, DOWN):
                sent(item, slot_of(z, yy, c), route)
            for k in range(1, nz):
                below(k, lambda zz, yy=yy: sent(item, slot_of(zz, yy, c), UP))
                above(k, lambda zz, yy=yy: sent(item, slot_of(zz, yy, c), DOWN))
        if both:
            sent(item, me, ACROSS)
        for zz in range(nz):
            if not both:
                sent(item, slot_of(zz, y, c), ACROSS)
            for yy in range(2):
                sent(item, slot_of(zz, yy, c), CORE)

    own = [
        pltpu.make_async_copy(w_query_ref, rows_of(WQ, me), local_sem.at[0]),
        pltpu.make_async_copy(
            w_key_ref.at[:, pl.ds(kv_start, kv_cols)],
            rows_of(WKV, me).at[:, pl.ds(0, kv_cols)],
            local_sem.at[1],
        ),
        pltpu.make_async_copy(
            w_value_ref.at[:, pl.ds(kv_start, kv_cols)],
            rows_of(WKV, me).at[:, pl.ds(kv_cols, kv_cols)],
            local_sem.at[2],
        ),
        pltpu.make_async_copy(w_out_ref, rows_of(WO, me), local_sem.at[3]),
    ]
    for one in own:
        one.start()

    barrier = pltpu.get_barrier_semaphore()

    def greet(blk, hd):
        pl.semaphore_signal(barrier, inc=1, device_id=(blk, hd), device_id_type=MESH)

    pl.when(z < nz - 1)(lambda: greet(me + 4, head))
    pl.when(z > 0)(lambda: greet(me - 4, head))
    greet(target(ACROSS)[0], head)
    greet(target(CORE)[0], head)
    peers = [lax.rem(head + d, heads) for d in range(1, heads)]
    for peer in peers:
        greet(me, peer)
    ends = jnp.where(z < nz - 1, 1, 0) + jnp.where(z > 0, 1, 0)
    pl.semaphore_wait(barrier, ends + 2 + len(peers))

    for one in own:
        one.wait()
    for route in (UP, DOWN, ACROSS):
        send(WQ, me, route)
    for route in (ACROSS, UP, DOWN, CORE):
        send(WKV, me, route)
    send(WQ, me, CORE)

    my_rows = pl.ds(pl.multiple_of(head * local_rows, local_rows), local_rows)
    floats = tokens_ref[...].astype(jnp.float32)
    normed[my_rows, :] = (
        floats
        * lax.rsqrt(jnp.mean(floats * floats, axis=1, keepdims=True) + eps_norm)
        * gain_ref[...]
    ).astype(jnp.bfloat16)

    there = slot_of(z, 1 - y, c)
    arrived(WKV, there)
    for route in (UP, DOWN, CORE):
        send(WKV, there, route)

    def norm_copy(d):
        return pltpu.make_async_remote_copy(
            src_ref=normed.at[my_rows],
            dst_ref=normed.at[my_rows],
            send_sem=norm_send.at[d],
            recv_sem=norm_recv.at[d],
            device_id=(me, peers[d]),
            device_id_type=MESH,
        )

    for d in range(len(peers)):
        norm_copy(d).start()

    for k in range(1, nz):
        z_step(WQ, k, y, (ACROSS, CORE))
        z_step(WKV, k, y, (CORE,))
        z_step(WKV, k, 1 - y, (CORE,))
        if k == nz - 1:
            for route in (UP, DOWN):
                send(WO, me, route)
        across(WQ, k - 1)
    send(WO, me, ACROSS)
    send(WO, me, CORE)
    across(WQ, nz - 1)
    for d in range(len(peers)):
        norm_copy(d).wait_recv()
    z_step(WO, 1, y)
    finish(WQ)
    finish(WKV)

    cosine, sine = cos_ref[...], sin_ref[...]

    def turn(values):
        return values * cosine + pltpu.roll(values, HD // 2, 1) * sine

    kv_rows = pl.ds(pl.multiple_of(me * group_rows, group_rows), group_rows)
    sums = jnp.dot(normed[...], wkv[...], preferred_element_type=jnp.float32)
    for g in range(kv_here):
        bias = k_bias_ref[:, pl.ds(pl.multiple_of(kv_start + g * HD, HD), HD)]
        kv[kv_rows, pl.ds(g * HD, HD)] = turn(sums[:, g * HD : (g + 1) * HD] + bias).astype(
            jnp.bfloat16
        )
        bias = v_bias_ref[:, pl.ds(pl.multiple_of(kv_start + g * HD, HD), HD)]
        at = kv_cols + g * HD
        kv[kv_rows, pl.ds(at, HD)] = (sums[:, at : at + HD] + bias).astype(jnp.bfloat16)

    for route in (UP, DOWN, ACROSS, CORE):
        send(KV, me, route)

    joined = 2 if heads_here % 2 == 0 else 1

    def project(n, carry):
        cols = pl.ds(pl.multiple_of(n * joined * HD, joined * HD), joined * HD)
        total = jnp.dot(normed[...], wq[:, cols], preferred_element_type=jnp.float32)
        total = total + q_bias_ref[:, cols]
        for j in range(joined):
            query[n * joined + j] = turn(total[:, j * HD : (j + 1) * HD]).astype(jnp.bfloat16)
        return carry

    lax.fori_loop(0, heads_here // joined, project, 0)

    for k in range(1, nz):
        z_step(KV, k, y, (ACROSS, CORE))
        if k + 1 < nz:
            z_step(WO, k + 1, y)
    for k in range(nz):
        across(KV, k)
    for k in range(1, nz):
        at_distance(k, lambda zz: send(WO, slot_of(zz, y, c), ACROSS))
        at_distance(k, lambda zz: send(WO, slot_of(zz, y, c), CORE))
    finish(KV)

    keys = kv.shape[0]
    span = block_width(keys, 512)
    stacked = per_kv * group_rows
    last_query = me * group_rows + group_rows - 1
    steps = last_query // span + 1

    for g in range(kv_here):
        q = query[g * per_kv : (g + 1) * per_kv].reshape(stacked, HD)

        def attend(j, state, q=q, g=g):
            top, total, acc = state
            at = pl.ds(pl.multiple_of(j * span, span), span)
            scores = (
                lax.dot_general(
                    q,
                    kv[at, pl.ds(g * HD, HD)],
                    (((1,), (1,)), ((), ())),
                    preferred_element_type=jnp.float32,
                )
                * scale
            )
            shape = (per_kv, group_rows, span)
            rows = lax.broadcasted_iota(jnp.int32, shape, 1).reshape(stacked, span)
            columns = lax.broadcasted_iota(jnp.int32, (stacked, span), 1)
            visible = columns + j * span <= rows + me * group_rows
            scores = jnp.where(visible, scores, masked_score)
            new_top = jnp.maximum(top, jnp.max(scores, axis=1, keepdims=True))
            weights = jnp.where(visible, jnp.exp(scores - new_top), 0.0)
            fade = jnp.exp(top - new_top)
            total = total * fade + jnp.sum(weights, axis=1, keepdims=True)
            acc = acc * fade + jnp.dot(
                weights.astype(jnp.bfloat16),
                kv[at, pl.ds(kv_cols + g * HD, HD)],
                preferred_element_type=jnp.float32,
            )
            return (new_top, total, acc)

        start = (
            jnp.full((stacked, 1), masked_score, jnp.float32),
            jnp.zeros((stacked, 1), jnp.float32),
            jnp.zeros((stacked, HD), jnp.float32),
        )
        top, total, acc = lax.fori_loop(0, steps, attend, start)
        result = (acc / total).astype(jnp.bfloat16)
        for r in range(per_kv):
            attended[:, pl.ds((g * per_kv + r) * HD, HD)] = result[
                r * group_rows : (r + 1) * group_rows
            ]

    for k in range(nz):
        across(WO, k)
    finish(WO)

    chunk = 256

    def produce(n, carry):
        cols = pl.ds(pl.multiple_of(n * chunk, chunk), chunk)
        result = lax.dot_general(
            attended[...],
            wo[cols, :],
            (((1,), (1,)), ((), ())),
            preferred_element_type=jnp.float32,
        )
        partial[:, cols] = result
        outgoing[:, cols] = result.astype(jnp.bfloat16)
        return carry

    lax.fori_loop(0, width // chunk, produce, 0)

    def sum_copy(d):
        rows = pl.ds(pl.multiple_of(peers[d] * local_rows, local_rows), local_rows)
        return pltpu.make_async_remote_copy(
            src_ref=outgoing.at[rows],
            dst_ref=incoming.at[d],
            send_sem=sum_send.at[d],
            recv_sem=sum_recv.at[d],
            device_id=(me, peers[d]),
            device_id_type=MESH,
        )

    for d in range(len(peers)):
        sum_copy(d).start()
    for item in (WQ, WKV, WO, KV):
        drain(item, item == WKV)
    for d in range(len(peers)):
        norm_copy(d).wait_send()
    for d in range(len(peers)):
        sum_copy(d).wait_recv()
    result = partial[my_rows, :]
    for d in range(len(peers)):
        result = result + incoming[d].astype(jnp.float32)
    out_ref[...] = result.astype(jnp.bfloat16)
    for d in range(len(peers)):
        sum_copy(d).wait_send()


def on_device(tokens, norm_gain, w_query, w_key, w_value, q_bias, k_bias, v_bias, w_out):
    blocks, heads = lax.axis_size("blk"), lax.axis_size("head")
    local_rows, width = tokens.shape
    group_rows = local_rows * heads
    heads_here = w_query.shape[1] // HD
    kv_here = max(1, heads_here // G)
    positions = lax.axis_index("blk") * group_rows + jnp.arange(group_rows, dtype=jnp.int32)
    half = HD // 2
    freq = theta_base ** (-(jnp.arange(half, dtype=jnp.float32) * 2.0 / HD))
    angles = positions.astype(jnp.float32)[:, None] * freq[None, :]
    cosine, sine = jnp.cos(angles), jnp.sin(angles)
    cosine = jnp.concatenate([cosine, cosine], axis=1)
    sine = jnp.concatenate([-sine, sine], axis=1)
    inner = heads_here * HD
    vmem = pl.BlockSpec(memory_space=pltpu.VMEM)
    hbm = pl.BlockSpec(memory_space=pl.ANY)
    others = max(1, heads - 1)
    bf16, f32 = jnp.bfloat16, jnp.float32
    return pl.pallas_call(
        functools.partial(kernel, (blocks, heads)),
        out_shape=jax.ShapeDtypeStruct((local_rows, width), bf16),
        in_specs=[vmem, vmem, hbm, hbm, hbm, vmem, vmem, vmem, hbm, vmem, vmem],
        out_specs=vmem,
        scratch_shapes=[
            pltpu.VMEM((width, inner), bf16),
            pltpu.VMEM((width, 2 * kv_here * HD), bf16),
            pltpu.VMEM((width, inner), bf16),
            pltpu.VMEM((blocks * group_rows, 2 * kv_here * HD), bf16),
            pltpu.VMEM((group_rows, width), bf16),
            pltpu.VMEM((heads_here, group_rows, HD), bf16),
            pltpu.VMEM((group_rows, inner), bf16),
            pltpu.VMEM((group_rows, width), f32),
            pltpu.VMEM((group_rows, width), bf16),
            pltpu.VMEM((others, local_rows, width), bf16),
            pltpu.SemaphoreType.DMA((4,)),
            pltpu.SemaphoreType.DMA((4, blocks, 4)),
            pltpu.SemaphoreType.DMA((4, blocks)),
            pltpu.SemaphoreType.DMA((others,)),
            pltpu.SemaphoreType.DMA((others,)),
            pltpu.SemaphoreType.DMA((others,)),
            pltpu.SemaphoreType.DMA((others,)),
        ],
        compiler_params=pltpu.CompilerParams(
            collective_id=0, has_side_effects=True, vmem_limit_bytes=60 * 1024 * 1024
        ),
    )(
        tokens,
        norm_gain[None, :],
        w_query,
        w_key,
        w_value,
        q_bias[None, :],
        k_bias[None, :],
        v_bias[None, :],
        w_out.T,
        cosine,
        sine,
    )


def solution(mesh):
    placed = (
        P(("blk", "head"), None),
        P(),
        P("blk", "head"),
        P("blk", None),
        P("blk", None),
        P("head"),
        P(),
        P(),
        P("head", "blk"),
    )
    return jax.shard_map(
        on_device, mesh=mesh, in_specs=placed, out_specs=P(("blk", "head"), None), check_vma=False
    )
```

```python
import functools
import math

import jax
import jax.numpy as jnp
from jax import lax
from jax.experimental import pallas as pl
from jax.experimental.pallas import tpu as pltpu
from jax.sharding import PartitionSpec as P

HD = 128
G = 6
MESH = pl.DeviceIdType.MESH

theta_base = 1000000.0
eps_norm = 1e-06
masked_score = -1e30

WQ, WKV, WO, KV = range(4)
UP, DOWN, ACROSS, CORE = range(4)


def block_width(rows, limit):
    width = min(rows, limit)
    while rows % width:
        width -= 1
    return width


def kernel(
    sizes,
    tokens_ref,
    gain_ref,
    w_query_ref,
    w_key_ref,
    w_value_ref,
    q_bias_ref,
    k_bias_ref,
    v_bias_ref,
    w_out_ref,
    cos_ref,
    sin_ref,
    out_ref,
    wq,
    wkv,
    wo,
    kv,
    normed,
    query,
    attended,
    partial,
    outgoing,
    incoming,
    local_sem,
    send_sem,
    recv_sem,
    norm_send,
    norm_recv,
    sum_send,
    sum_recv,
):
    blocks, heads = sizes
    nz = blocks // 4
    me = lax.axis_index("blk")
    head = lax.axis_index("head")
    z, y, c = me // 4, (me // 2) % 2, me % 2
    local_rows, width = tokens_ref.shape
    group_rows = local_rows * heads
    heads_here = wq.shape[1] // HD
    kv_here = wkv.shape[1] // (2 * HD)
    per_kv = heads_here // kv_here
    kv_cols = kv_here * HD
    kv_start = pl.multiple_of((head * heads_here // G) * HD, HD)
    buffers = {WQ: wq, WKV: wkv, WO: wo, KV: kv}
    scale = 1.0 / math.sqrt(HD)

    def slot_of(zz, yy, cc):
        return (zz * 2 + yy) * 2 + cc

    def rows_of(item, slot):
        each = buffers[item].shape[0] // blocks
        return buffers[item].at[pl.ds(pl.multiple_of(slot * each, each), each)]

    def target(route):
        step = {UP: 4, DOWN: -4, ACROSS: 2 - 4 * y, CORE: 1 - 2 * c}[route]
        return (me + step, head)

    def copy(item, slot, route):
        part = rows_of(item, slot)
        return pltpu.make_async_remote_copy(
            src_ref=part,
            dst_ref=part,
            send_sem=send_sem.at[item, slot, route],
            recv_sem=recv_sem.at[item, slot],
            device_id=target(route),
            device_id_type=MESH,
        )

    def send(item, slot, route):
        if route == UP:
            pl.when(z < nz - 1)(lambda: copy(item, slot, route).start())
        elif route == DOWN:
            pl.when(z > 0)(lambda: copy(item, slot, route).start())
        else:
            copy(item, slot, route).start()

    def sent(item, slot, route):
        if route == UP:
            pl.when(z < nz - 1)(lambda: copy(item, slot, route).wait_send())
        elif route == DOWN:
            pl.when(z > 0)(lambda: copy(item, slot, route).wait_send())
        else:
            copy(item, slot, route).wait_send()

    def arrived(item, slot):
        copy(item, slot, CORE).wait_recv()

    def below(k, act):
        pl.when(z >= k)(lambda: act(z - k))

    def above(k, act):
        pl.when(z + k < nz)(lambda: act(z + k))

    def z_step(item, k, yy, then=()):
        def from_below(zz):
            slot = slot_of(zz, yy, c)
            arrived(item, slot)
            for route in (UP,) + then:
                send(item, slot, route)

        def from_above(zz):
            slot = slot_of(zz, yy, c)
            arrived(item, slot)
            for route in (DOWN,) + then:
                send(item, slot, route)

        below(k, from_below)
        above(k, from_above)

    def at_distance(k, act):
        if k == 0:
            act(z)
        else:
            below(k, act)
            above(k, act)

    def across(item, k):
        def act(zz):
            slot = slot_of(zz, 1 - y, c)
            arrived(item, slot)
            send(item, slot, CORE)

        at_distance(k, act)

    def finish(item):
        for zz in range(nz):
            for yy in range(2):
                arrived(item, slot_of(zz, yy, 1 - c))

    def drain(item, both):
        for yy in (y, 1 - y) if both else (y,):
            for route in (UP, DOWN):
                sent(item, slot_of(z, yy, c), route)
            for k in range(1, nz):
                below(k, lambda zz, yy=yy: sent(item, slot_of(zz, yy, c), UP))
                above(k, lambda zz, yy=yy: sent(item, slot_of(zz, yy, c), DOWN))
        if both:
            sent(item, me, ACROSS)
        for zz in range(nz):
            if not both:
                sent(item, slot_of(zz, y, c), ACROSS)
            for yy in range(2):
                sent(item, slot_of(zz, yy, c), CORE)

    own = [
        pltpu.make_async_copy(w_query_ref, rows_of(WQ, me), local_sem.at[0]),
        pltpu.make_async_copy(
            w_key_ref.at[:, pl.ds(kv_start, kv_cols)],
            rows_of(WKV, me).at[:, pl.ds(0, kv_cols)],
            local_sem.at[1],
        ),
        pltpu.make_async_copy(
            w_value_ref.at[:, pl.ds(kv_start, kv_cols)],
            rows_of(WKV, me).at[:, pl.ds(kv_cols, kv_cols)],
            local_sem.at[2],
        ),
        pltpu.make_async_copy(w_out_ref, rows_of(WO, me), local_sem.at[3]),
    ]
    for one in own:
        one.start()

    barrier = pltpu.get_barrier_semaphore()

    def greet(blk, hd):
        pl.semaphore_signal(barrier, inc=1, device_id=(blk, hd), device_id_type=MESH)

    pl.when(z < nz - 1)(lambda: greet(me + 4, head))
    pl.when(z > 0)(lambda: greet(me - 4, head))
    greet(target(ACROSS)[0], head)
    greet(target(CORE)[0], head)
    peers = [lax.rem(head + d, heads) for d in range(1, heads)]
    for peer in peers:
        greet(me, peer)
    ends = jnp.where(z < nz - 1, 1, 0) + jnp.where(z > 0, 1, 0)
    pl.semaphore_wait(barrier, ends + 2 + len(peers))

    own[1].wait()
    own[2].wait()
    for route in (ACROSS, UP, DOWN, CORE):
        send(WKV, me, route)
    own[0].wait()
    own[3].wait()
    for route in (ACROSS, CORE):
        send(WQ, me, route)
    for route in (ACROSS, CORE):
        send(WO, me, route)

    my_rows = pl.ds(pl.multiple_of(head * local_rows, local_rows), local_rows)
    floats = tokens_ref[...].astype(jnp.float32)
    normed[my_rows, :] = (
        floats
        * lax.rsqrt(jnp.mean(floats * floats, axis=1, keepdims=True) + eps_norm)
        * gain_ref[...]
    ).astype(jnp.bfloat16)

    there = slot_of(z, 1 - y, c)
    arrived(WKV, there)
    for route in (UP, DOWN, CORE):
        send(WKV, there, route)

    def norm_copy(d):
        return pltpu.make_async_remote_copy(
            src_ref=normed.at[my_rows],
            dst_ref=normed.at[my_rows],
            send_sem=norm_send.at[d],
            recv_sem=norm_recv.at[d],
            device_id=(me, peers[d]),
            device_id_type=MESH,
        )

    for d in range(len(peers)):
        norm_copy(d).start()

    for k in range(1, nz):
        z_step(WKV, k, y, (CORE,))
        z_step(WKV, k, 1 - y, (CORE,))
        if k == max(1, nz - 2):
            for route in (UP, DOWN):
                send(WQ, me, route)
    if nz == 1:
        for route in (UP, DOWN):
            send(WQ, me, route)
    for d in range(len(peers)):
        norm_copy(d).wait_recv()
    finish(WKV)

    cosine, sine = cos_ref[...], sin_ref[...]

    def turn(values):
        return values * cosine + pltpu.roll(values, HD // 2, 1) * sine

    kv_rows = pl.ds(pl.multiple_of(me * group_rows, group_rows), group_rows)
    sums = jnp.dot(normed[...], wkv[...], preferred_element_type=jnp.float32)
    for g in range(kv_here):
        bias = k_bias_ref[:, pl.ds(pl.multiple_of(kv_start + g * HD, HD), HD)]
        kv[kv_rows, pl.ds(g * HD, HD)] = turn(sums[:, g * HD : (g + 1) * HD] + bias).astype(
            jnp.bfloat16
        )
        bias = v_bias_ref[:, pl.ds(pl.multiple_of(kv_start + g * HD, HD), HD)]
        at = kv_cols + g * HD
        kv[kv_rows, pl.ds(at, HD)] = (sums[:, at : at + HD] + bias).astype(jnp.bfloat16)

    across(WQ, 0)
    for route in (UP, DOWN, ACROSS, CORE):
        send(KV, me, route)

    for k in range(1, nz):
        z_step(WQ, k, y, (ACROSS, CORE))
        if k == max(1, nz - 2):
            for route in (UP, DOWN):
                send(WO, me, route)
        z_step(KV, k, y, (ACROSS, CORE))
    if nz == 1:
        for route in (UP, DOWN):
            send(WO, me, route)
    for k in range(1, nz):
        if k == nz - 1:
            z_step(WO, 1, y, (ACROSS, CORE))
        across(WQ, k)
    for k in range(nz):
        across(KV, k)
    finish(WQ)
    finish(KV)

    joined = 2 if heads_here % 2 == 0 else 1

    def project(n, carry):
        cols = pl.ds(pl.multiple_of(n * joined * HD, joined * HD), joined * HD)
        total = jnp.dot(normed[...], wq[:, cols], preferred_element_type=jnp.float32)
        total = total + q_bias_ref[:, cols]
        for j in range(joined):
            query[n * joined + j] = turn(total[:, j * HD : (j + 1) * HD]).astype(jnp.bfloat16)
        return carry

    lax.fori_loop(0, heads_here // joined, project, 0)

    keys = kv.shape[0]
    span = block_width(keys, 512)
    stacked = per_kv * group_rows
    last_query = me * group_rows + group_rows - 1
    steps = last_query // span + 1

    for g in range(kv_here):
        q = query[g * per_kv : (g + 1) * per_kv].reshape(stacked, HD)

        def attend(j, state, q=q, g=g):
            top, total, acc = state
            at = pl.ds(pl.multiple_of(j * span, span), span)
            scores = (
                lax.dot_general(
                    q,
                    kv[at, pl.ds(g * HD, HD)],
                    (((1,), (1,)), ((), ())),
                    preferred_element_type=jnp.float32,
                )
                * scale
            )
            shape = (per_kv, group_rows, span)
            rows = lax.broadcasted_iota(jnp.int32, shape, 1).reshape(stacked, span)
            columns = lax.broadcasted_iota(jnp.int32, (stacked, span), 1)
            visible = columns + j * span <= rows + me * group_rows
            scores = jnp.where(visible, scores, masked_score)
            new_top = jnp.maximum(top, jnp.max(scores, axis=1, keepdims=True))
            weights = jnp.where(visible, jnp.exp(scores - new_top), 0.0)
            fade = jnp.exp(top - new_top)
            total = total * fade + jnp.sum(weights, axis=1, keepdims=True)
            acc = acc * fade + jnp.dot(
                weights.astype(jnp.bfloat16),
                kv[at, pl.ds(kv_cols + g * HD, HD)],
                preferred_element_type=jnp.float32,
            )
            return (new_top, total, acc)

        start = (
            jnp.full((stacked, 1), masked_score, jnp.float32),
            jnp.zeros((stacked, 1), jnp.float32),
            jnp.zeros((stacked, HD), jnp.float32),
        )
        top, total, acc = lax.fori_loop(0, steps, attend, start)
        result = (acc / total).astype(jnp.bfloat16)
        for r in range(per_kv):
            attended[:, pl.ds((g * per_kv + r) * HD, HD)] = result[
                r * group_rows : (r + 1) * group_rows
            ]
        if 2 + g < nz:
            z_step(WO, 2 + g, y, (ACROSS, CORE))

    for k in range(2 + kv_here, nz):
        z_step(WO, k, y, (ACROSS, CORE))

    each = wo.shape[0] // blocks
    grouped = (4 * each) % HD == 0
    groups = nz if grouped else 1
    chunk = width // groups

    def sum_copy(d, i, start):
        rows = pl.ds(pl.multiple_of(peers[d] * local_rows, local_rows), local_rows)
        cols = pl.ds(pl.multiple_of(start, HD), chunk)
        return pltpu.make_async_remote_copy(
            src_ref=outgoing.at[rows, cols],
            dst_ref=incoming.at[d, :, cols],
            send_sem=sum_send.at[d, i],
            recv_sem=sum_recv.at[d, i],
            device_id=(me, peers[d]),
            device_id_type=MESH,
        )

    def produce(start, size):
        cols = pl.ds(pl.multiple_of(start, HD), size)
        result = lax.dot_general(
            attended[...],
            wo[cols, :],
            (((1,), (1,)), ((), ())),
            preferred_element_type=jnp.float32,
        )
        partial[:, cols] = result
        outgoing[:, cols] = result.astype(jnp.bfloat16)

    def place(i):
        way = 1 - 2 * (z // max(1, nz // 2)) if nz > 1 else 1
        return lax.rem(z + way * i + nz, nz)

    if grouped:

        def produce_group(i, carry):
            zz = place(i)
            slot = slot_of(zz, 1 - y, c)
            arrived(WO, slot)
            send(WO, slot, CORE)
            for yy in range(2):
                arrived(WO, slot_of(zz, yy, 1 - c))
            produce(zz * 4 * each, chunk)
            for d in range(len(peers)):
                sum_copy(d, i, zz * chunk).start()
            return carry

        lax.fori_loop(0, nz, produce_group, 0)
    else:
        for k in range(nz):
            across(WO, k)
        finish(WO)
        part = 256
        lax.fori_loop(0, width // part, lambda n, carry: (produce(n * part, part), carry)[1], 0)
        for d in range(len(peers)):
            sum_copy(d, 0, 0).start()

    for item in (WQ, WKV, WO, KV):
        drain(item, item == WKV)
    for d in range(len(peers)):
        norm_copy(d).wait_send()

    def collect(i, carry):
        start = place(i) * chunk if grouped else 0
        cols = pl.ds(pl.multiple_of(start, HD), chunk)
        for d in range(len(peers)):
            sum_copy(d, i, start).wait_recv()
        result = partial[my_rows, cols]
        for d in range(len(peers)):
            result = result + incoming[d, :, cols].astype(jnp.float32)
        out_ref[:, cols] = result.astype(jnp.bfloat16)
        for d in range(len(peers)):
            sum_copy(d, i, start).wait_send()
        return carry

    lax.fori_loop(0, groups, collect, 0)


def on_device(tokens, norm_gain, w_query, w_key, w_value, q_bias, k_bias, v_bias, w_out):
    blocks, heads = lax.axis_size("blk"), lax.axis_size("head")
    local_rows, width = tokens.shape
    group_rows = local_rows * heads
    heads_here = w_query.shape[1] // HD
    kv_here = max(1, heads_here // G)
    positions = lax.axis_index("blk") * group_rows + jnp.arange(group_rows, dtype=jnp.int32)
    half = HD // 2
    freq = theta_base ** (-(jnp.arange(half, dtype=jnp.float32) * 2.0 / HD))
    angles = positions.astype(jnp.float32)[:, None] * freq[None, :]
    cosine, sine = jnp.cos(angles), jnp.sin(angles)
    cosine = jnp.concatenate([cosine, cosine], axis=1)
    sine = jnp.concatenate([-sine, sine], axis=1)
    inner = heads_here * HD
    vmem = pl.BlockSpec(memory_space=pltpu.VMEM)
    hbm = pl.BlockSpec(memory_space=pl.ANY)
    others = max(1, heads - 1)
    bf16, f32 = jnp.bfloat16, jnp.float32
    return pl.pallas_call(
        functools.partial(kernel, (blocks, heads)),
        out_shape=jax.ShapeDtypeStruct((local_rows, width), bf16),
        in_specs=[vmem, vmem, hbm, hbm, hbm, vmem, vmem, vmem, hbm, vmem, vmem],
        out_specs=vmem,
        scratch_shapes=[
            pltpu.VMEM((width, inner), bf16),
            pltpu.VMEM((width, 2 * kv_here * HD), bf16),
            pltpu.VMEM((width, inner), bf16),
            pltpu.VMEM((blocks * group_rows, 2 * kv_here * HD), bf16),
            pltpu.VMEM((group_rows, width), bf16),
            pltpu.VMEM((heads_here, group_rows, HD), bf16),
            pltpu.VMEM((group_rows, inner), bf16),
            pltpu.VMEM((group_rows, width), f32),
            pltpu.VMEM((group_rows, width), bf16),
            pltpu.VMEM((others, local_rows, width), bf16),
            pltpu.SemaphoreType.DMA((4,)),
            pltpu.SemaphoreType.DMA((4, blocks, 4)),
            pltpu.SemaphoreType.DMA((4, blocks)),
            pltpu.SemaphoreType.DMA((others,)),
            pltpu.SemaphoreType.DMA((others,)),
            pltpu.SemaphoreType.DMA((others, blocks // 4)),
            pltpu.SemaphoreType.DMA((others, blocks // 4)),
        ],
        compiler_params=pltpu.CompilerParams(
            collective_id=0, has_side_effects=True, vmem_limit_bytes=60 * 1024 * 1024
        ),
    )(
        tokens,
        norm_gain[None, :],
        w_query,
        w_key,
        w_value,
        q_bias[None, :],
        k_bias[None, :],
        v_bias[None, :],
        w_out.T,
        cosine,
        sine,
    )


def solution(mesh):
    placed = (
        P(("blk", "head"), None),
        P(),
        P("blk", "head"),
        P("blk", None),
        P("blk", None),
        P("head"),
        P(),
        P(),
        P("head", "blk"),
    )
    return jax.shard_map(
        on_device, mesh=mesh, in_specs=placed, out_specs=P(("blk", "head"), None), check_vma=False
    )
```

```python
import functools
import math

import jax
import jax.numpy as jnp
from jax import lax
from jax.experimental import pallas as pl
from jax.experimental.pallas import tpu as pltpu
from jax.sharding import PartitionSpec as P

HD = 128
G = 6
MESH = pl.DeviceIdType.MESH

theta_base = 1000000.0
eps_norm = 1e-06
masked_score = -1e30

WQ, WKV, WO, KV, WQ_TAIL, WO_TAIL = range(6)
UP, DOWN, ACROSS, CORE = range(4)


def block_width(rows, limit):
    width = min(rows, limit)
    while rows % width:
        width -= 1
    return width


def kernel(
    sizes,
    tokens_ref,
    gain_ref,
    w_query_ref,
    w_key_ref,
    w_value_ref,
    q_bias_ref,
    k_bias_ref,
    v_bias_ref,
    w_out_ref,
    cos_ref,
    sin_ref,
    out_ref,
    wq,
    wkv,
    wo,
    kv,
    normed,
    query,
    attended,
    partial,
    outgoing,
    incoming,
    local_sem,
    send_sem,
    recv_sem,
    norm_send,
    norm_recv,
    sum_send,
    sum_recv,
):
    blocks, heads = sizes
    nz = blocks // 4
    me = lax.axis_index("blk")
    head = lax.axis_index("head")
    z, y, c = me // 4, (me // 2) % 2, me % 2
    local_rows, width = tokens_ref.shape
    group_rows = local_rows * heads
    heads_here = wq.shape[1] // HD
    kv_here = wkv.shape[1] // (2 * HD)
    per_kv = heads_here // kv_here
    kv_cols = kv_here * HD
    kv_start = pl.multiple_of((head * heads_here // G) * HD, HD)
    buffers = {WQ: wq, WKV: wkv, WO: wo, KV: kv, WQ_TAIL: wq, WO_TAIL: wo}
    queries, outs = (WQ, WQ_TAIL), (WO, WO_TAIL)
    scale = 1.0 / math.sqrt(HD)

    def slot_of(zz, yy, cc):
        return (zz * 2 + yy) * 2 + cc

    def rows_of(item, slot):
        each = buffers[item].shape[0] // blocks
        first, size = 0, each
        if item in queries + outs:
            cut = each // 2 // 16 * 16
            first, size = (0, cut) if item in (WQ, WO) else (cut, each - cut)
        return buffers[item].at[pl.ds(pl.multiple_of(slot * each + first, 16), size)]

    def whole_rows(ref):
        each = ref.shape[0] // blocks
        return ref.at[pl.ds(pl.multiple_of(me * each, each), each)]

    def target(route):
        step = {UP: 4, DOWN: -4, ACROSS: 2 - 4 * y, CORE: 1 - 2 * c}[route]
        return (me + step, head)

    def copy(item, slot, route):
        part = rows_of(item, slot)
        return pltpu.make_async_remote_copy(
            src_ref=part,
            dst_ref=part,
            send_sem=send_sem.at[item, slot, route],
            recv_sem=recv_sem.at[item, slot],
            device_id=target(route),
            device_id_type=MESH,
        )

    def send(item, slot, route):
        if route == UP:
            pl.when(z < nz - 1)(lambda: copy(item, slot, route).start())
        elif route == DOWN:
            pl.when(z > 0)(lambda: copy(item, slot, route).start())
        else:
            copy(item, slot, route).start()

    def sent(item, slot, route):
        if route == UP:
            pl.when(z < nz - 1)(lambda: copy(item, slot, route).wait_send())
        elif route == DOWN:
            pl.when(z > 0)(lambda: copy(item, slot, route).wait_send())
        else:
            copy(item, slot, route).wait_send()

    def arrived(item, slot):
        copy(item, slot, CORE).wait_recv()

    def below(k, act):
        pl.when(z >= k)(lambda: act(z - k))

    def above(k, act):
        pl.when(z + k < nz)(lambda: act(z + k))

    def z_step(item, k, yy, then=()):
        def from_below(zz):
            slot = slot_of(zz, yy, c)
            arrived(item, slot)
            for route in (UP,) + then:
                send(item, slot, route)

        def from_above(zz):
            slot = slot_of(zz, yy, c)
            arrived(item, slot)
            for route in (DOWN,) + then:
                send(item, slot, route)

        below(k, from_below)
        above(k, from_above)

    def at_distance(k, act):
        if k == 0:
            act(z)
        else:
            below(k, act)
            above(k, act)

    def across(item, k):
        def act(zz):
            slot = slot_of(zz, 1 - y, c)
            arrived(item, slot)
            send(item, slot, CORE)

        at_distance(k, act)

    def finish(item):
        for zz in range(nz):
            for yy in range(2):
                arrived(item, slot_of(zz, yy, 1 - c))

    def drain(item, both):
        for yy in (y, 1 - y) if both else (y,):
            for route in (UP, DOWN):
                sent(item, slot_of(z, yy, c), route)
            for k in range(1, nz):
                below(k, lambda zz, yy=yy: sent(item, slot_of(zz, yy, c), UP))
                above(k, lambda zz, yy=yy: sent(item, slot_of(zz, yy, c), DOWN))
        if both:
            sent(item, me, ACROSS)
        for zz in range(nz):
            if not both:
                sent(item, slot_of(zz, y, c), ACROSS)
            for yy in range(2):
                sent(item, slot_of(zz, yy, c), CORE)

    own = [
        pltpu.make_async_copy(w_query_ref, whole_rows(wq), local_sem.at[0]),
        pltpu.make_async_copy(
            w_key_ref.at[:, pl.ds(kv_start, kv_cols)],
            rows_of(WKV, me).at[:, pl.ds(0, kv_cols)],
            local_sem.at[1],
        ),
        pltpu.make_async_copy(
            w_value_ref.at[:, pl.ds(kv_start, kv_cols)],
            rows_of(WKV, me).at[:, pl.ds(kv_cols, kv_cols)],
            local_sem.at[2],
        ),
        pltpu.make_async_copy(w_out_ref, whole_rows(wo), local_sem.at[3]),
    ]
    for one in own:
        one.start()

    barrier = pltpu.get_barrier_semaphore()

    def greet(blk, hd):
        pl.semaphore_signal(barrier, inc=1, device_id=(blk, hd), device_id_type=MESH)

    pl.when(z < nz - 1)(lambda: greet(me + 4, head))
    pl.when(z > 0)(lambda: greet(me - 4, head))
    greet(target(ACROSS)[0], head)
    greet(target(CORE)[0], head)
    peers = [lax.rem(head + d, heads) for d in range(1, heads)]
    for peer in peers:
        greet(me, peer)
    ends = jnp.where(z < nz - 1, 1, 0) + jnp.where(z > 0, 1, 0)
    pl.semaphore_wait(barrier, ends + 2 + len(peers))

    own[1].wait()
    own[2].wait()
    for route in (ACROSS, UP, DOWN, CORE):
        send(WKV, me, route)
    own[0].wait()
    own[3].wait()
    for item in queries + outs:
        for route in (ACROSS, CORE):
            send(item, me, route)

    my_rows = pl.ds(pl.multiple_of(head * local_rows, local_rows), local_rows)
    floats = tokens_ref[...].astype(jnp.float32)
    normed[my_rows, :] = (
        floats
        * lax.rsqrt(jnp.mean(floats * floats, axis=1, keepdims=True) + eps_norm)
        * gain_ref[...]
    ).astype(jnp.bfloat16)

    there = slot_of(z, 1 - y, c)
    arrived(WKV, there)
    for route in (UP, DOWN, CORE):
        send(WKV, there, route)

    def norm_copy(d):
        return pltpu.make_async_remote_copy(
            src_ref=normed.at[my_rows],
            dst_ref=normed.at[my_rows],
            send_sem=norm_send.at[d],
            recv_sem=norm_recv.at[d],
            device_id=(me, peers[d]),
            device_id_type=MESH,
        )

    for d in range(len(peers)):
        norm_copy(d).start()

    for k in range(1, nz):
        z_step(WKV, k, y, (CORE,))
        z_step(WKV, k, 1 - y, (CORE,))
        if k == max(1, nz - 2):
            for item in queries:
                for route in (UP, DOWN):
                    send(item, me, route)
    for d in range(len(peers)):
        norm_copy(d).wait_recv()
    finish(WKV)

    cosine, sine = cos_ref[...], sin_ref[...]

    def turn(values):
        return values * cosine + pltpu.roll(values, HD // 2, 1) * sine

    kv_rows = pl.ds(pl.multiple_of(me * group_rows, group_rows), group_rows)
    sums = jnp.dot(normed[...], wkv[...], preferred_element_type=jnp.float32)
    for g in range(kv_here):
        bias = k_bias_ref[:, pl.ds(pl.multiple_of(kv_start + g * HD, HD), HD)]
        kv[kv_rows, pl.ds(g * HD, HD)] = turn(sums[:, g * HD : (g + 1) * HD] + bias).astype(
            jnp.bfloat16
        )
        bias = v_bias_ref[:, pl.ds(pl.multiple_of(kv_start + g * HD, HD), HD)]
        at = kv_cols + g * HD
        kv[kv_rows, pl.ds(at, HD)] = (sums[:, at : at + HD] + bias).astype(jnp.bfloat16)

    for item in queries:
        across(item, 0)
    for route in (UP, DOWN, ACROSS, CORE):
        send(KV, me, route)

    for k in range(1, nz):
        for item in queries:
            z_step(item, k, y, (ACROSS, CORE))
        z_step(KV, k, y, (ACROSS, CORE))
        if k == max(1, nz - 2):
            for item in outs:
                for route in (UP, DOWN):
                    send(item, me, route)
    for k in range(1, nz):
        if k == nz - 1:
            for item in outs:
                z_step(item, 1, y, (ACROSS, CORE))
        for item in queries:
            across(item, k)
    for k in range(nz):
        across(KV, k)
    for item in queries + (KV,):
        finish(item)

    joined = 2 if heads_here % 2 == 0 else 1

    def project(n, carry):
        cols = pl.ds(pl.multiple_of(n * joined * HD, joined * HD), joined * HD)
        total = jnp.dot(normed[...], wq[:, cols], preferred_element_type=jnp.float32)
        total = total + q_bias_ref[:, cols]
        for j in range(joined):
            query[n * joined + j] = turn(total[:, j * HD : (j + 1) * HD]).astype(jnp.bfloat16)
        return carry

    lax.fori_loop(0, heads_here // joined, project, 0)

    if nz > 2:
        for item in outs:
            z_step(item, 2, y, (ACROSS, CORE))

    keys = kv.shape[0]
    span = block_width(keys, 512)
    stacked = per_kv * group_rows
    last_query = me * group_rows + group_rows - 1
    steps = last_query // span + 1

    for g in range(kv_here):
        q = query[g * per_kv : (g + 1) * per_kv].reshape(stacked, HD)

        def attend(j, state, q=q, g=g):
            top, total, acc = state
            at = pl.ds(pl.multiple_of(j * span, span), span)
            scores = (
                lax.dot_general(
                    q,
                    kv[at, pl.ds(g * HD, HD)],
                    (((1,), (1,)), ((), ())),
                    preferred_element_type=jnp.float32,
                )
                * scale
            )
            shape = (per_kv, group_rows, span)
            rows = lax.broadcasted_iota(jnp.int32, shape, 1).reshape(stacked, span)
            columns = lax.broadcasted_iota(jnp.int32, (stacked, span), 1)
            visible = columns + j * span <= rows + me * group_rows
            scores = jnp.where(visible, scores, masked_score)
            new_top = jnp.maximum(top, jnp.max(scores, axis=1, keepdims=True))
            weights = jnp.where(visible, jnp.exp(scores - new_top), 0.0)
            fade = jnp.exp(top - new_top)
            total = total * fade + jnp.sum(weights, axis=1, keepdims=True)
            acc = acc * fade + jnp.dot(
                weights.astype(jnp.bfloat16),
                kv[at, pl.ds(kv_cols + g * HD, HD)],
                preferred_element_type=jnp.float32,
            )
            return (new_top, total, acc)

        start = (
            jnp.full((stacked, 1), masked_score, jnp.float32),
            jnp.zeros((stacked, 1), jnp.float32),
            jnp.zeros((stacked, HD), jnp.float32),
        )
        top, total, acc = lax.fori_loop(0, steps, attend, start)
        result = (acc / total).astype(jnp.bfloat16)
        for r in range(per_kv):
            attended[:, pl.ds((g * per_kv + r) * HD, HD)] = result[
                r * group_rows : (r + 1) * group_rows
            ]
        for k in range(3, nz):
            if g == 0:
                z_step(WO, k, y, (ACROSS, CORE))
    for k in range(3, nz):
        z_step(WO_TAIL, k, y, (ACROSS, CORE))

    each = wo.shape[0] // blocks
    grouped = (4 * each) % HD == 0
    groups = nz if grouped else 1
    chunk = width // groups

    def sum_copy(d, i, start):
        rows = pl.ds(pl.multiple_of(peers[d] * local_rows, local_rows), local_rows)
        cols = pl.ds(pl.multiple_of(start, HD), chunk)
        return pltpu.make_async_remote_copy(
            src_ref=outgoing.at[rows, cols],
            dst_ref=incoming.at[d, :, cols],
            send_sem=sum_send.at[d, i],
            recv_sem=sum_recv.at[d, i],
            device_id=(me, peers[d]),
            device_id_type=MESH,
        )

    def produce(start, size):
        cols = pl.ds(pl.multiple_of(start, HD), size)
        result = lax.dot_general(
            attended[...],
            wo[cols, :],
            (((1,), (1,)), ((), ())),
            preferred_element_type=jnp.float32,
        )
        partial[:, cols] = result
        outgoing[:, cols] = result.astype(jnp.bfloat16)

    def place(i):
        way = 1 - 2 * (z // max(1, nz // 2)) if nz > 1 else 1
        return lax.rem(z + way * i + nz, nz)

    if grouped:

        def produce_group(i, carry):
            zz = place(i)
            slot = slot_of(zz, 1 - y, c)
            for item in outs:
                arrived(item, slot)
                send(item, slot, CORE)
            for item in outs:
                for yy in range(2):
                    arrived(item, slot_of(zz, yy, 1 - c))
            produce(zz * 4 * each, chunk)
            for d in range(len(peers)):
                sum_copy(d, i, zz * chunk).start()
            return carry

        lax.fori_loop(0, nz, produce_group, 0)
    else:
        for item in outs:
            for k in range(nz):
                across(item, k)
            finish(item)
        part = 256
        lax.fori_loop(0, width // part, lambda n, carry: (produce(n * part, part), carry)[1], 0)
        for d in range(len(peers)):
            sum_copy(d, 0, 0).start()

    for item in queries + outs + (WKV, KV):
        drain(item, item == WKV)
    for d in range(len(peers)):
        norm_copy(d).wait_send()

    def collect(i, carry):
        start = place(i) * chunk if grouped else 0
        cols = pl.ds(pl.multiple_of(start, HD), chunk)
        for d in range(len(peers)):
            sum_copy(d, i, start).wait_recv()
        result = partial[my_rows, cols]
        for d in range(len(peers)):
            result = result + incoming[d, :, cols].astype(jnp.float32)
        out_ref[:, cols] = result.astype(jnp.bfloat16)
        for d in range(len(peers)):
            sum_copy(d, i, start).wait_send()
        return carry

    lax.fori_loop(0, groups, collect, 0)


def on_device(tokens, norm_gain, w_query, w_key, w_value, q_bias, k_bias, v_bias, w_out):
    blocks, heads = lax.axis_size("blk"), lax.axis_size("head")
    local_rows, width = tokens.shape
    group_rows = local_rows * heads
    heads_here = w_query.shape[1] // HD
    kv_here = max(1, heads_here // G)
    positions = lax.axis_index("blk") * group_rows + jnp.arange(group_rows, dtype=jnp.int32)
    half = HD // 2
    freq = theta_base ** (-(jnp.arange(half, dtype=jnp.float32) * 2.0 / HD))
    angles = positions.astype(jnp.float32)[:, None] * freq[None, :]
    cosine, sine = jnp.cos(angles), jnp.sin(angles)
    cosine = jnp.concatenate([cosine, cosine], axis=1)
    sine = jnp.concatenate([-sine, sine], axis=1)
    inner = heads_here * HD
    vmem = pl.BlockSpec(memory_space=pltpu.VMEM)
    hbm = pl.BlockSpec(memory_space=pl.ANY)
    others = max(1, heads - 1)
    bf16, f32 = jnp.bfloat16, jnp.float32
    return pl.pallas_call(
        functools.partial(kernel, (blocks, heads)),
        out_shape=jax.ShapeDtypeStruct((local_rows, width), bf16),
        in_specs=[vmem, vmem, hbm, hbm, hbm, vmem, vmem, vmem, hbm, vmem, vmem],
        out_specs=vmem,
        scratch_shapes=[
            pltpu.VMEM((width, inner), bf16),
            pltpu.VMEM((width, 2 * kv_here * HD), bf16),
            pltpu.VMEM((width, inner), bf16),
            pltpu.VMEM((blocks * group_rows, 2 * kv_here * HD), bf16),
            pltpu.VMEM((group_rows, width), bf16),
            pltpu.VMEM((heads_here, group_rows, HD), bf16),
            pltpu.VMEM((group_rows, inner), bf16),
            pltpu.VMEM((group_rows, width), f32),
            pltpu.VMEM((group_rows, width), bf16),
            pltpu.VMEM((others, local_rows, width), bf16),
            pltpu.SemaphoreType.DMA((4,)),
            pltpu.SemaphoreType.DMA((6, blocks, 4)),
            pltpu.SemaphoreType.DMA((6, blocks)),
            pltpu.SemaphoreType.DMA((others,)),
            pltpu.SemaphoreType.DMA((others,)),
            pltpu.SemaphoreType.DMA((others, blocks // 4)),
            pltpu.SemaphoreType.DMA((others, blocks // 4)),
        ],
        compiler_params=pltpu.CompilerParams(
            collective_id=0, has_side_effects=True, vmem_limit_bytes=60 * 1024 * 1024
        ),
    )(
        tokens,
        norm_gain[None, :],
        w_query,
        w_key,
        w_value,
        q_bias[None, :],
        k_bias[None, :],
        v_bias[None, :],
        w_out.T,
        cosine,
        sine,
    )


def solution(mesh):
    placed = (
        P(("blk", "head"), None),
        P(),
        P("blk", "head"),
        P("blk", None),
        P("blk", None),
        P("head"),
        P(),
        P(),
        P("head", "blk"),
    )
    return jax.shard_map(
        on_device, mesh=mesh, in_specs=placed, out_specs=P(("blk", "head"), None), check_vma=False
    )
```

```python
import functools
import math

import jax
import jax.numpy as jnp
from jax import lax
from jax.experimental import pallas as pl
from jax.experimental.pallas import tpu as pltpu
from jax.sharding import PartitionSpec as P

HD = 128
G = 6
MESH = pl.DeviceIdType.MESH

theta_base = 1000000.0
eps_norm = 1e-06
masked_score = -1e30

WQ, WKV, WO, KV, WQ_TAIL, WO_TAIL, WO_SIDE = range(7)
UP, DOWN, ACROSS, CORE = range(4)


def block_width(rows, limit):
    width = min(rows, limit)
    while rows % width:
        width -= 1
    return width


def kernel(
    sizes,
    tokens_ref,
    gain_ref,
    w_query_ref,
    w_key_ref,
    w_value_ref,
    q_bias_ref,
    k_bias_ref,
    v_bias_ref,
    w_out_ref,
    cos_ref,
    sin_ref,
    out_ref,
    wq,
    wkv,
    wo,
    kv,
    normed,
    query,
    attended,
    partial,
    outgoing,
    incoming,
    local_sem,
    send_sem,
    recv_sem,
    norm_send,
    norm_recv,
    sum_send,
    sum_recv,
):
    blocks, heads = sizes
    nz = blocks // 4
    me = lax.axis_index("blk")
    head = lax.axis_index("head")
    z, y, c = me // 4, (me // 2) % 2, me % 2
    local_rows, width = tokens_ref.shape
    group_rows = local_rows * heads
    heads_here = wq.shape[1] // HD
    kv_here = wkv.shape[1] // (2 * HD)
    per_kv = heads_here // kv_here
    kv_cols = kv_here * HD
    kv_start = pl.multiple_of((head * heads_here // G) * HD, HD)
    buffers = {WQ: wq, WKV: wkv, WO: wo, KV: kv, WQ_TAIL: wq, WO_TAIL: wo, WO_SIDE: wo}
    queries, outs = (WQ, WQ_TAIL), (WO, WO_TAIL)
    scale = 1.0 / math.sqrt(HD)
    side = 16

    def slot_of(zz, yy, cc):
        return (zz * 2 + yy) * 2 + cc

    def rows_of(item, slot):
        each = buffers[item].shape[0] // blocks
        first, size = 0, each
        if item in queries + outs:
            cut = each // 2 // 16 * 16
            end = each - side if item == WO_TAIL else each
            first, size = (0, cut) if item in (WQ, WO) else (cut, end - cut)
        if item == WO_SIDE:
            first, size = each - side, side
        return buffers[item].at[pl.ds(pl.multiple_of(slot * each + first, 16), size)]

    def whole_rows(ref):
        each = ref.shape[0] // blocks
        return ref.at[pl.ds(pl.multiple_of(me * each, each), each)]

    def target(route):
        step = {UP: 4, DOWN: -4, ACROSS: 2 - 4 * y, CORE: 1 - 2 * c}[route]
        return (me + step, head)

    def copy(item, slot, route):
        part = rows_of(item, slot)
        return pltpu.make_async_remote_copy(
            src_ref=part,
            dst_ref=part,
            send_sem=send_sem.at[item, slot, route],
            recv_sem=recv_sem.at[item, slot],
            device_id=target(route),
            device_id_type=MESH,
        )

    def send(item, slot, route):
        if route == UP:
            pl.when(z < nz - 1)(lambda: copy(item, slot, route).start())
        elif route == DOWN:
            pl.when(z > 0)(lambda: copy(item, slot, route).start())
        else:
            copy(item, slot, route).start()

    def sent(item, slot, route):
        if route == UP:
            pl.when(z < nz - 1)(lambda: copy(item, slot, route).wait_send())
        elif route == DOWN:
            pl.when(z > 0)(lambda: copy(item, slot, route).wait_send())
        else:
            copy(item, slot, route).wait_send()

    def arrived(item, slot):
        copy(item, slot, CORE).wait_recv()

    def below(k, act):
        pl.when(z >= k)(lambda: act(z - k))

    def above(k, act):
        pl.when(z + k < nz)(lambda: act(z + k))

    def z_step(item, k, yy, then=()):
        def from_below(zz):
            slot = slot_of(zz, yy, c)
            arrived(item, slot)
            for route in (UP,) + then:
                send(item, slot, route)

        def from_above(zz):
            slot = slot_of(zz, yy, c)
            arrived(item, slot)
            for route in (DOWN,) + then:
                send(item, slot, route)

        below(k, from_below)
        above(k, from_above)

    def at_distance(k, act):
        if k == 0:
            act(z)
        else:
            below(k, act)
            above(k, act)

    def across(item, k):
        def act(zz):
            slot = slot_of(zz, 1 - y, c)
            arrived(item, slot)
            send(item, slot, CORE)

        at_distance(k, act)

    def finish(item):
        for zz in range(nz):
            for yy in range(2):
                arrived(item, slot_of(zz, yy, 1 - c))

    def drain(item, both):
        for yy in (y, 1 - y) if both else (y,):
            for route in (UP, DOWN):
                sent(item, slot_of(z, yy, c), route)
            for k in range(1, nz):
                below(k, lambda zz, yy=yy: sent(item, slot_of(zz, yy, c), UP))
                above(k, lambda zz, yy=yy: sent(item, slot_of(zz, yy, c), DOWN))
        if both:
            sent(item, me, ACROSS)
        for zz in range(nz):
            if not both:
                sent(item, slot_of(zz, y, c), ACROSS)
            for yy in range(2):
                sent(item, slot_of(zz, yy, c), CORE)

    own = [
        pltpu.make_async_copy(w_query_ref, whole_rows(wq), local_sem.at[0]),
        pltpu.make_async_copy(
            w_key_ref.at[:, pl.ds(kv_start, kv_cols)],
            rows_of(WKV, me).at[:, pl.ds(0, kv_cols)],
            local_sem.at[1],
        ),
        pltpu.make_async_copy(
            w_value_ref.at[:, pl.ds(kv_start, kv_cols)],
            rows_of(WKV, me).at[:, pl.ds(kv_cols, kv_cols)],
            local_sem.at[2],
        ),
        pltpu.make_async_copy(w_out_ref, whole_rows(wo), local_sem.at[3]),
    ]
    for one in own:
        one.start()

    barrier = pltpu.get_barrier_semaphore()

    def greet(blk, hd):
        pl.semaphore_signal(barrier, inc=1, device_id=(blk, hd), device_id_type=MESH)

    pl.when(z < nz - 1)(lambda: greet(me + 4, head))
    pl.when(z > 0)(lambda: greet(me - 4, head))
    greet(target(ACROSS)[0], head)
    greet(target(CORE)[0], head)
    peers = [lax.rem(head + d, heads) for d in range(1, heads)]
    for peer in peers:
        greet(me, peer)
    ends = jnp.where(z < nz - 1, 1, 0) + jnp.where(z > 0, 1, 0)
    pl.semaphore_wait(barrier, ends + 2 + len(peers))

    own[1].wait()
    own[2].wait()
    for route in (ACROSS, UP, DOWN, CORE):
        send(WKV, me, route)
    own[0].wait()
    own[3].wait()
    for item in queries + (WO_SIDE,) + outs:
        for route in (ACROSS, CORE):
            send(item, me, route)

    my_rows = pl.ds(pl.multiple_of(head * local_rows, local_rows), local_rows)
    floats = tokens_ref[...].astype(jnp.float32)
    normed[my_rows, :] = (
        floats
        * lax.rsqrt(jnp.mean(floats * floats, axis=1, keepdims=True) + eps_norm)
        * gain_ref[...]
    ).astype(jnp.bfloat16)

    there = slot_of(z, 1 - y, c)
    arrived(WKV, there)
    for route in (UP, DOWN, CORE):
        send(WKV, there, route)

    def norm_copy(d):
        return pltpu.make_async_remote_copy(
            src_ref=normed.at[my_rows],
            dst_ref=normed.at[my_rows],
            send_sem=norm_send.at[d],
            recv_sem=norm_recv.at[d],
            device_id=(me, peers[d]),
            device_id_type=MESH,
        )

    for d in range(len(peers)):
        norm_copy(d).start()

    for k in range(1, nz):
        z_step(WKV, k, y, (CORE,))
        z_step(WKV, k, 1 - y, (CORE,))
        if k == max(1, nz - 2):
            for item in queries:
                for route in (UP, DOWN):
                    send(item, me, route)
    for d in range(len(peers)):
        norm_copy(d).wait_recv()
    finish(WKV)

    cosine, sine = cos_ref[...], sin_ref[...]

    def turn(values):
        return values * cosine + pltpu.roll(values, HD // 2, 1) * sine

    kv_rows = pl.ds(pl.multiple_of(me * group_rows, group_rows), group_rows)
    sums = jnp.dot(normed[...], wkv[...], preferred_element_type=jnp.float32)
    for g in range(kv_here):
        bias = k_bias_ref[:, pl.ds(pl.multiple_of(kv_start + g * HD, HD), HD)]
        kv[kv_rows, pl.ds(g * HD, HD)] = turn(sums[:, g * HD : (g + 1) * HD] + bias).astype(
            jnp.bfloat16
        )
        bias = v_bias_ref[:, pl.ds(pl.multiple_of(kv_start + g * HD, HD), HD)]
        at = kv_cols + g * HD
        kv[kv_rows, pl.ds(at, HD)] = (sums[:, at : at + HD] + bias).astype(jnp.bfloat16)

    for item in queries:
        across(item, 0)
    for route in (UP, DOWN, ACROSS, CORE):
        send(KV, me, route)

    for k in range(1, nz):
        for item in queries:
            z_step(item, k, y, (ACROSS, CORE))
        z_step(KV, k, y, (ACROSS, CORE))
        if k == max(1, nz - 2):
            for item in (WO, WO_SIDE, WO_TAIL):
                for route in (UP, DOWN):
                    send(item, me, route)
            arrived(WO_SIDE, there)
            for route in (UP, DOWN, CORE):
                send(WO_SIDE, there, route)
    for k in range(1, nz):
        if k == nz - 1:
            for item in outs:
                z_step(item, 1, y, (ACROSS, CORE))
            for yy in (y, 1 - y):
                z_step(WO_SIDE, 1, yy, (CORE,))
        for item in queries:
            across(item, k)
    for k in range(nz):
        across(KV, k)
    for item in queries + (KV,):
        finish(item)

    joined = 2 if heads_here % 2 == 0 else 1

    def project(n, carry):
        cols = pl.ds(pl.multiple_of(n * joined * HD, joined * HD), joined * HD)
        total = jnp.dot(normed[...], wq[:, cols], preferred_element_type=jnp.float32)
        total = total + q_bias_ref[:, cols]
        for j in range(joined):
            query[n * joined + j] = turn(total[:, j * HD : (j + 1) * HD]).astype(jnp.bfloat16)
        return carry

    lax.fori_loop(0, heads_here // joined, project, 0)

    if nz > 2:
        for item in outs:
            z_step(item, 2, y, (ACROSS, CORE))
        for yy in (y, 1 - y):
            z_step(WO_SIDE, 2, yy, (CORE,))

    keys = kv.shape[0]
    span = block_width(keys, 512)
    stacked = per_kv * group_rows
    last_query = me * group_rows + group_rows - 1
    steps = last_query // span + 1

    for g in range(kv_here):
        q = query[g * per_kv : (g + 1) * per_kv].reshape(stacked, HD)

        def attend(j, state, q=q, g=g):
            top, total, acc = state
            at = pl.ds(pl.multiple_of(j * span, span), span)
            scores = (
                lax.dot_general(
                    q,
                    kv[at, pl.ds(g * HD, HD)],
                    (((1,), (1,)), ((), ())),
                    preferred_element_type=jnp.float32,
                )
                * scale
            )
            shape = (per_kv, group_rows, span)
            rows = lax.broadcasted_iota(jnp.int32, shape, 1).reshape(stacked, span)
            columns = lax.broadcasted_iota(jnp.int32, (stacked, span), 1)
            visible = columns + j * span <= rows + me * group_rows
            scores = jnp.where(visible, scores, masked_score)
            new_top = jnp.maximum(top, jnp.max(scores, axis=1, keepdims=True))
            weights = jnp.where(visible, jnp.exp(scores - new_top), 0.0)
            fade = jnp.exp(top - new_top)
            total = total * fade + jnp.sum(weights, axis=1, keepdims=True)
            acc = acc * fade + jnp.dot(
                weights.astype(jnp.bfloat16),
                kv[at, pl.ds(kv_cols + g * HD, HD)],
                preferred_element_type=jnp.float32,
            )
            return (new_top, total, acc)

        start = (
            jnp.full((stacked, 1), masked_score, jnp.float32),
            jnp.zeros((stacked, 1), jnp.float32),
            jnp.zeros((stacked, HD), jnp.float32),
        )
        top, total, acc = lax.fori_loop(0, steps, attend, start)
        result = (acc / total).astype(jnp.bfloat16)
        for r in range(per_kv):
            attended[:, pl.ds((g * per_kv + r) * HD, HD)] = result[
                r * group_rows : (r + 1) * group_rows
            ]
        for k in range(3, nz):
            if g == 0:
                z_step(WO, k, y, (ACROSS, CORE))
    for k in range(3, nz):
        z_step(WO_TAIL, k, y, (ACROSS, CORE))
        for yy in (y, 1 - y):
            z_step(WO_SIDE, k, yy, (CORE,))

    each = wo.shape[0] // blocks
    grouped = (4 * each) % HD == 0
    groups = nz if grouped else 1
    chunk = width // groups

    def sum_copy(d, i, start):
        rows = pl.ds(pl.multiple_of(peers[d] * local_rows, local_rows), local_rows)
        cols = pl.ds(pl.multiple_of(start, HD), chunk)
        return pltpu.make_async_remote_copy(
            src_ref=outgoing.at[rows, cols],
            dst_ref=incoming.at[d, :, cols],
            send_sem=sum_send.at[d, i],
            recv_sem=sum_recv.at[d, i],
            device_id=(me, peers[d]),
            device_id_type=MESH,
        )

    def produce(start, size):
        cols = pl.ds(pl.multiple_of(start, HD), size)
        result = lax.dot_general(
            attended[...],
            wo[cols, :],
            (((1,), (1,)), ((), ())),
            preferred_element_type=jnp.float32,
        )
        partial[:, cols] = result
        outgoing[:, cols] = result.astype(jnp.bfloat16)

    def place(i):
        way = 1 - 2 * (z // max(1, nz // 2)) if nz > 1 else 1
        return lax.rem(z + way * i + nz, nz)

    if grouped:

        def produce_group(i, carry):
            zz = place(i)
            slot = slot_of(zz, 1 - y, c)
            for item in outs:
                arrived(item, slot)
                send(item, slot, CORE)
            for item in outs + (WO_SIDE,):
                for yy in range(2):
                    arrived(item, slot_of(zz, yy, 1 - c))
            produce(zz * 4 * each, chunk)
            for d in range(len(peers)):
                sum_copy(d, i, zz * chunk).start()
            return carry

        lax.fori_loop(0, nz, produce_group, 0)
    else:
        for item in outs:
            for k in range(nz):
                across(item, k)
            finish(item)
        finish(WO_SIDE)
        part = 256
        lax.fori_loop(0, width // part, lambda n, carry: (produce(n * part, part), carry)[1], 0)
        for d in range(len(peers)):
            sum_copy(d, 0, 0).start()

    for item in queries + outs + (WKV, KV, WO_SIDE):
        drain(item, item in (WKV, WO_SIDE))
    for d in range(len(peers)):
        norm_copy(d).wait_send()

    def collect(i, carry):
        start = place(i) * chunk if grouped else 0
        cols = pl.ds(pl.multiple_of(start, HD), chunk)
        for d in range(len(peers)):
            sum_copy(d, i, start).wait_recv()
        result = partial[my_rows, cols]
        for d in range(len(peers)):
            result = result + incoming[d, :, cols].astype(jnp.float32)
        out_ref[:, cols] = result.astype(jnp.bfloat16)
        for d in range(len(peers)):
            sum_copy(d, i, start).wait_send()
        return carry

    lax.fori_loop(0, groups, collect, 0)


def on_device(tokens, norm_gain, w_query, w_key, w_value, q_bias, k_bias, v_bias, w_out):
    blocks, heads = lax.axis_size("blk"), lax.axis_size("head")
    local_rows, width = tokens.shape
    group_rows = local_rows * heads
    heads_here = w_query.shape[1] // HD
    kv_here = max(1, heads_here // G)
    positions = lax.axis_index("blk") * group_rows + jnp.arange(group_rows, dtype=jnp.int32)
    half = HD // 2
    freq = theta_base ** (-(jnp.arange(half, dtype=jnp.float32) * 2.0 / HD))
    angles = positions.astype(jnp.float32)[:, None] * freq[None, :]
    cosine, sine = jnp.cos(angles), jnp.sin(angles)
    cosine = jnp.concatenate([cosine, cosine], axis=1)
    sine = jnp.concatenate([-sine, sine], axis=1)
    inner = heads_here * HD
    vmem = pl.BlockSpec(memory_space=pltpu.VMEM)
    hbm = pl.BlockSpec(memory_space=pl.ANY)
    others = max(1, heads - 1)
    bf16, f32 = jnp.bfloat16, jnp.float32
    return pl.pallas_call(
        functools.partial(kernel, (blocks, heads)),
        out_shape=jax.ShapeDtypeStruct((local_rows, width), bf16),
        in_specs=[vmem, vmem, hbm, hbm, hbm, vmem, vmem, vmem, hbm, vmem, vmem],
        out_specs=vmem,
        scratch_shapes=[
            pltpu.VMEM((width, inner), bf16),
            pltpu.VMEM((width, 2 * kv_here * HD), bf16),
            pltpu.VMEM((width, inner), bf16),
            pltpu.VMEM((blocks * group_rows, 2 * kv_here * HD), bf16),
            pltpu.VMEM((group_rows, width), bf16),
            pltpu.VMEM((heads_here, group_rows, HD), bf16),
            pltpu.VMEM((group_rows, inner), bf16),
            pltpu.VMEM((group_rows, width), f32),
            pltpu.VMEM((group_rows, width), bf16),
            pltpu.VMEM((others, local_rows, width), bf16),
            pltpu.SemaphoreType.DMA((4,)),
            pltpu.SemaphoreType.DMA((7, blocks, 4)),
            pltpu.SemaphoreType.DMA((7, blocks)),
            pltpu.SemaphoreType.DMA((others,)),
            pltpu.SemaphoreType.DMA((others,)),
            pltpu.SemaphoreType.DMA((others, blocks // 4)),
            pltpu.SemaphoreType.DMA((others, blocks // 4)),
        ],
        compiler_params=pltpu.CompilerParams(
            collective_id=0, has_side_effects=True, vmem_limit_bytes=60 * 1024 * 1024
        ),
    )(
        tokens,
        norm_gain[None, :],
        w_query,
        w_key,
        w_value,
        q_bias[None, :],
        k_bias[None, :],
        v_bias[None, :],
        w_out.T,
        cosine,
        sine,
    )


def solution(mesh):
    placed = (
        P(("blk", "head"), None),
        P(),
        P("blk", "head"),
        P("blk", None),
        P("blk", None),
        P("head"),
        P(),
        P(),
        P("head", "blk"),
    )
    return jax.shard_map(
        on_device, mesh=mesh, in_specs=placed, out_specs=P(("blk", "head"), None), check_vma=False
    )
```
